32 devices in a mesh: batch: 4 (over x, core), cache: 8 (over z, y).
Axes of the slice: x: 2, y: 2, z: 4, core: 2. Of those that a mesh axis runs over, the one named last changes fastest.
Arguments:
- hidden_in: bfloat16 [32, 4096], P('batch'), may hold values from -6 to 6
- attn_gain: bfloat16 [4096], replicated, may hold values from 0.25 to 1.75
- w_query: bfloat16 [4096, 4096], P(None, 'cache'), may hold values from -0.09375 to 0.09375
- w_key: bfloat16 [4096, 1024], P(None, 'cache'), may hold values from -0.09375 to 0.09375
- w_value: bfloat16 [4096, 1024], P(None, 'cache'), may hold values from -0.09375 to 0.09375
- key_cache: bfloat16 [32, 1024, 1024], P('batch', 'cache'), may hold values from -400 to 400, as said below
- value_cache: bfloat16 [32, 1024, 1024], P('batch', 'cache'), may hold values from -6 to 6
- write_pos: int32 [32], P('batch'), may hold values from 0 to 3071, as said below
- cache_len: int32 [32], P('batch'), may hold values from 0 to 1023, as said below
- w_out: bfloat16 [4096, 4096], P('cache'), may hold values from -0.125 to 0.125
- mlp_gain: bfloat16 [4096], replicated, may hold values from 0.25 to 1.75
- w_gate: bfloat16 [4096, 7168], P(None, 'cache'), may hold values from -0.09375 to 0.09375
- w_up: bfloat16 [4096, 7168], P(None, 'cache'), may hold values from -0.09375 to 0.09375
- w_down: bfloat16 [7168, 4096], P('cache'), may hold values from -0.09375 to 0.09375
Outputs:
- hidden_out: bfloat16 [32, 4096], P('batch', 'cache')
The draws below stay inside these ranges and needn't reach their ends.
Inputs may be any that keep to these rules, and one draw needn't show every extreme that they name: `key_cache`: keys of earlier tokens are finite reals. `write_pos`: positions of the new tokens; the largest value occurs in every draw. cache_len never exceeds write_pos; both 0 and 1023 occur in every draw, and many sequences attend fewer than 1023 earlier tokens.
All inputs are finite; a program needn't handle non-finite values.
Results may differ from the reference program's by a relative error of at most 0.017.
Values may be sent and summed in bfloat16 or wider, within the bound.
A program may use at most 64 MiB of HBM per device.

```python
import jax
import jax.numpy as jnp
from jax import lax

D = 4096
HEADS = 32
KV_HEADS = 8
HEAD_DIM = 128
FFW = 7168
SEQS = 32
CACHE_SLOTS = 1024


def position_pair(key):
    inner = jax.random.fold_in(key, 11)
    first, second, third = jax.random.split(inner, 3)
    position = jax.random.randint(first, (SEQS,), 0, 3 * CACHE_SLOTS)
    position = position.at[0].set(3 * CACHE_SLOTS - 1)
    longest = jnp.minimum(position, CACHE_SLOTS - 1)
    partial_len = jax.random.randint(second, (SEQS,), 0, longest + 1)
    picked = jax.random.randint(third, (SEQS,), 0, 2)
    length = jnp.where(picked == 1, longest, partial_len)
    length = length.at[0].set(CACHE_SLOTS - 1)
    length = length.at[1].set(0)
    return (position.astype(jnp.int32), length.astype(jnp.int32))


def draw_write_pos(key, part):
    return position_pair(key)[0]


def draw_cache_len(key, part):
    return position_pair(key)[1]


def draw_key_cache(key, part):
    inner = jax.random.fold_in(key, 23)
    first = jax.random.fold_in(inner, 0)
    base = jnp.clip(jax.random.normal(first, (SEQS, CACHE_SLOTS, KV_HEADS * HEAD_DIM), jnp.float32), -6.0, 6.0)
    return base.astype(jnp.bfloat16)


def spiked(entries, rng, source, target, parts, factor):
    owner, partner = [(jnp.arange(entries.shape[dim]) // (entries.shape[dim] // parts)).reshape([-1 if axis == dim else 1 for axis in range(entries.ndim)]) for dim in (source, target)]
    chosen = jax.random.permutation(rng, parts)[partner]
    strong = (owner == chosen) | (owner == (partner + parts // 2) % parts)
    return jnp.where(strong, factor * entries, entries)


def block_levels(own_key, dims, pieces, least, top_value):
    level, own = 1.0, jax.random.fold_in(own_key, 6)
    for axis_at, parts in pieces:
        heights = jnp.exp(jax.random.uniform(jax.random.fold_in(own, axis_at), (parts,), jnp.float32, least / len(pieces), top_value / len(pieces)))
        level = level * jnp.repeat(heights, dims[axis_at] // parts).reshape([-1 if axis == axis_at else 1 for axis in range(len(dims))])
    return level


def normal_values(own_key, dims, deviation, most, cuts=(), kind=jnp.bfloat16):
    factor_of = block_levels(own_key, dims, cuts, -0.22, 0.18) if cuts else 1.0
    drawn = jax.random.normal(own_key, dims, jnp.float32) * deviation * factor_of
    return jnp.minimum(jnp.maximum(drawn, -most), most).astype(kind)


def heavy_noise(key, shape, scale, bound, shards, heavy, kind=jnp.bfloat16):
    values = scale * jax.random.normal(key, shape, jnp.float32)
    if shards:
        values = values * block_levels(key, shape, shards, -0.22, 0.18)
    return jnp.clip(spiked(values, jax.random.fold_in(key, 3), *heavy), -bound, bound).astype(kind)


def setup_inputs(seed: int = 0) -> dict:
    streams_of = jax.random.split(jax.random.key(seed), 15)
    hidden_in = normal_values(streams_of[0], (SEQS, D), 1.0, 6.0, ((0, 4),))
    attn_gain = jnp.clip(1.0 + 0.15 * jax.random.normal(streams_of[1], (D,), jnp.float32), 0.25, 1.75).astype(jnp.bfloat16)
    w_query = normal_values(streams_of[2], (D, HEADS * HEAD_DIM), D ** -0.5, 0.09375, ((1, 8),))
    w_key = normal_values(streams_of[3], (D, KV_HEADS * HEAD_DIM), D ** -0.5, 0.09375, ((1, 8),))
    w_value = normal_values(streams_of[4], (D, KV_HEADS * HEAD_DIM), D ** -0.5, 0.09375, ((1, 8),))
    key_cache = draw_key_cache(jax.random.fold_in(streams_of[14], 71), 0)
    value_cache = normal_values(streams_of[6], (SEQS, CACHE_SLOTS, KV_HEADS * HEAD_DIM), 1.0, 6.0, ((0, 4), (1, 8)))
    write_pos = draw_write_pos(jax.random.fold_in(streams_of[14], 71), 0)
    cache_len = draw_cache_len(jax.random.fold_in(streams_of[14], 71), 0)
    w_out = heavy_noise(streams_of[9], (HEADS * HEAD_DIM, D), (HEADS * HEAD_DIM) ** -0.5, 0.125, ((0, 8),), (0, 1, 8, 2.0))
    mlp_gain = jnp.clip(1.0 + 0.15 * jax.random.normal(streams_of[10], (D,), jnp.float32), 0.25, 1.75).astype(jnp.bfloat16)
    w_gate = normal_values(streams_of[11], (D, FFW), D ** -0.5, 0.09375, ((1, 8),))
    w_up = normal_values(streams_of[12], (D, FFW), D ** -0.5, 0.09375, ((1, 8),))
    w_down = heavy_noise(streams_of[13], (FFW, D), FFW ** -0.5, 0.09375, ((0, 8),), (0, 1, 8, 2.0))
    return dict(hidden_in=hidden_in, attn_gain=attn_gain, w_query=w_query, w_key=w_key, w_value=w_value, key_cache=key_cache, value_cache=value_cache, write_pos=write_pos, cache_len=cache_len, w_out=w_out, mlp_gain=mlp_gain, w_gate=w_gate, w_up=w_up, w_down=w_down)


def rms_norm(values, gain):
    wide = values.astype(jnp.float32)
    spread = lax.optimization_barrier(jnp.mean(wide * wide, axis=-1, keepdims=True))
    return (wide * lax.rsqrt(spread + 1e-05) * gain.astype(jnp.float32)).astype(jnp.bfloat16)

def rotate(heads, position):
    half = heads.shape[-1] // 2
    freq = 10000.0 ** (-(jnp.arange(half, dtype=jnp.float32) * 2.0 / heads.shape[-1]))
    angle = position.astype(jnp.float32)[:, None] * freq[None, :]
    cosine = jnp.cos(angle)[:, None, :]
    sine = jnp.sin(angle)[:, None, :]
    first = heads[..., :half]
    second = heads[..., half:]
    return jnp.concatenate([first * cosine - second * sine, second * cosine + first * sine], axis=-1)

def reference(hidden_in, attn_gain, w_query, w_key, w_value, key_cache, value_cache, write_pos, cache_len, w_out, mlp_gain, w_gate, w_up, w_down):
    seqs = hidden_in.shape[0]
    group = HEADS // KV_HEADS
    normed = rms_norm(hidden_in, attn_gain)
    query_raw = jnp.dot(normed, w_query, preferred_element_type=jnp.float32).astype(jnp.bfloat16)
    key_raw = jnp.dot(normed, w_key, preferred_element_type=jnp.float32).astype(jnp.bfloat16)
    value_new = jnp.dot(normed, w_value, preferred_element_type=jnp.float32).astype(jnp.bfloat16)
    query = rotate(query_raw.astype(jnp.float32).reshape(seqs, HEADS, HEAD_DIM), write_pos).astype(jnp.bfloat16)
    fresh_key_row = rotate(key_raw.astype(jnp.float32).reshape(seqs, KV_HEADS, HEAD_DIM), write_pos).astype(jnp.bfloat16)
    slots = jnp.arange(CACHE_SLOTS, dtype=jnp.int32)
    dist = (write_pos[:, None] - 1 - slots[None, :]) % CACHE_SLOTS + 1
    valid = dist <= cache_len[:, None]
    scale = 1.0 / HEAD_DIM ** 0.5

    def one_sequence(items):
        qrow, keys, values, knew, vnew, keep = items
        qwide = qrow.astype(jnp.float32).reshape(KV_HEADS, group, HEAD_DIM)
        kwide = keys.astype(jnp.float32).reshape(CACHE_SLOTS, KV_HEADS, HEAD_DIM)
        vwide = values.astype(jnp.float32).reshape(CACHE_SLOTS, KV_HEADS, HEAD_DIM)
        scores = jnp.einsum('kgd,wkd->kgw', qwide, kwide) * scale
        own = jnp.einsum('kgd,kd->kg', qwide, knew.astype(jnp.float32)) * scale
        scores = jnp.where(keep[None, None, :], scores, -1e+30)
        top = jnp.maximum(lax.optimization_barrier(jnp.max(scores, axis=-1)), own)
        weights = jnp.where(keep[None, None, :], jnp.exp(scores - top[..., None]), 0.0)
        own_weight = jnp.exp(own - top)
        total = lax.optimization_barrier(jnp.sum(weights, axis=-1)) + own_weight
        low = lax.optimization_barrier(weights.astype(jnp.bfloat16)).astype(jnp.float32)
        own_low = lax.optimization_barrier(own_weight.astype(jnp.bfloat16)).astype(jnp.float32)
        reduced_total = jnp.einsum('kgw,wkd->kgd', low, vwide) + own_low[..., None] * vnew.astype(jnp.float32)[:, None, :]
        return (reduced_total / total[..., None]).reshape(HEADS * HEAD_DIM).astype(jnp.bfloat16)
    attended = lax.map(one_sequence, (query, key_cache, value_cache, fresh_key_row, value_new.reshape(seqs, KV_HEADS, HEAD_DIM), valid))
    projected = jnp.dot(attended, w_out, preferred_element_type=jnp.float32)
    mid = (hidden_in.astype(jnp.float32) + projected).astype(jnp.bfloat16)
    normed_mid = rms_norm(mid, mlp_gain)
    gate = jnp.dot(normed_mid, w_gate, preferred_element_type=jnp.float32)
    upper = jnp.dot(normed_mid, w_up, preferred_element_type=jnp.float32)
    act = (jax.nn.silu(gate) * upper).astype(jnp.bfloat16)
    down = jnp.dot(act, w_down, preferred_element_type=jnp.float32)
    return (mid.astype(jnp.float32) + down).astype(jnp.bfloat16)
```

```python
import functools

import jax
import jax.numpy as jnp
import numpy as np
from jax import lax
from jax.experimental import pallas as pl
from jax.experimental.pallas import tpu as pltpu
from jax.sharding import PartitionSpec as P

HEADS = 32
KV_HEADS = 8
HEAD_DIM = 128
GROUP = HEADS // KV_HEADS
EPS = 1e-05
LOW = -1e30
MESH = pl.DeviceIdType.MESH
F32 = jnp.float32
BF16 = jnp.bfloat16


def row_dot(left, right):
    return jnp.dot(left, right, preferred_element_type=F32)


def layer_kernel(
    ncache,
    qchunks,
    pos_s,
    len_s,
    freq_h,
    hid_h,
    again_h,
    wq_h,
    wk_h,
    wv_h,
    kc_h,
    vc_h,
    wo_h,
    mgain_h,
    wg_h,
    wu_h,
    wd_h,
    out_ref,
    freq,
    hid,
    again,
    wq,
    wk,
    wv,
    kc,
    vc,
    wo,
    mgain,
    wg,
    wu,
    wd,
    q_all,
    o_send,
    o_recv,
    l_send,
    l_recv,
    p_send,
    p_recv,
    m_send,
    m_recv,
    d_send,
    d_recv,
    local_sem,
    q_sem,
    send_sem,
    recv_sem,
):
    me = lax.axis_index("cache")
    line = lax.axis_index("batch")
    seqs, width = hid.shape
    feat = width // ncache
    slots = kc.shape[1]
    window = slots * ncache
    depth = width // qchunks
    scale = 1.0 / HEAD_DIM**0.5
    peers = [lax.rem(me + s, ncache) for s in range(ncache)]
    sources = [lax.rem(me - s + ncache, ncache) for s in range(ncache)]
    half = ncache // 2
    far_first = sorted(range(1, ncache), key=lambda s: (-min(s, ncache - s), s))
    near_first = far_first[::-1]

    def load(i, src, dst):
        copy = pltpu.make_async_copy(src, dst, local_sem.at[i])
        copy.start()
        return copy

    c_hid = load(0, hid_h, hid)
    c_again = load(1, again_h, again)
    c_freq = load(2, freq_h, freq)
    c_mgain = load(3, mgain_h, mgain)
    c_q = []
    for i in range(qchunks):
        rows = pl.ds(i * depth, depth)
        copy = pltpu.make_async_copy(wq_h.at[rows, :], wq.at[rows, :], q_sem.at[i])
        copy.start()
        c_q.append(copy)
    c_k = load(4, wk_h, wk)
    c_v = load(5, wv_h, wv)
    c_kc = load(6, kc_h, kc)
    c_vc = load(7, vc_h, vc)
    c_wo = load(8, wo_h, wo)

    barrier = pltpu.get_barrier_semaphore()
    for s in range(1, ncache):
        pl.semaphore_signal(barrier, inc=1, device_id=(line, peers[s]), device_id_type=MESH)

    def send(phase, s, src, dst):
        copy = pltpu.make_async_remote_copy(
            src_ref=src,
            dst_ref=dst,
            send_sem=send_sem.at[phase, s],
            recv_sem=recv_sem.at[phase, s],
            device_id=(line, peers[s]),
            device_id_type=MESH,
        )
        copy.start()
        return copy

    c_hid.wait()
    c_again.wait()
    c_freq.wait()
    wide = hid[...].astype(F32)
    spread = jnp.mean(wide * wide, axis=-1, keepdims=True)
    normed = (wide * lax.rsqrt(spread + EPS) * again[...].astype(F32)).astype(BF16)

    row8 = lax.broadcasted_iota(jnp.int32, (seqs, HEAD_DIM), 0)
    lane8 = lax.broadcasted_iota(jnp.int32, (seqs, HEAD_DIM), 1)
    position = jnp.zeros((seqs, HEAD_DIM), jnp.int32)
    for b in range(seqs):
        position = jnp.where(row8 == b, pos_s[b], position)
    angle = position.astype(F32) * freq[...]
    cosine = jnp.cos(angle)
    sine = jnp.sin(angle)
    sine = jnp.where(lane8 < HEAD_DIM // 2, -sine, sine)

    def rotated(x):
        x = x.astype(BF16).astype(F32)
        return (x * cosine + pltpu.roll(x, HEAD_DIM // 2, 1) * sine).astype(BF16)

    rows2 = 2 * GROUP * seqs
    row_seq = lax.broadcasted_iota(jnp.int32, (rows2, slots), 0) % seqs
    slot = lax.broadcasted_iota(jnp.int32, (rows2, slots), 1) + me * slots
    newest = jnp.zeros((rows2, slots), jnp.int32)
    length = jnp.zeros((rows2, slots), jnp.int32)
    for b in range(seqs):
        newest = jnp.where(row_seq == b, lax.rem(pos_s[b] - 1 + window, window), newest)
        length = jnp.where(row_seq == b, len_s[b], length)
    dist = newest - slot
    dist = jnp.where(dist < 0, dist + window, dist) + 1
    valid = dist <= length

    q_raw = jnp.zeros((seqs, wq.shape[1]), F32)
    for i in range(qchunks):
        c_q[i].wait()
        q_raw += row_dot(normed[:, i * depth : (i + 1) * depth], wq[i * depth : (i + 1) * depth, :])
    c_wg = load(9, wg_h, wg)
    c_wu = load(10, wu_h, wu)
    c_wd = load(11, wd_h, wd)
    query = jnp.concatenate(
        [rotated(q_raw[:, g * HEAD_DIM : (g + 1) * HEAD_DIM]) for g in range(GROUP)], axis=1
    )
    q_all[me] = query
    pl.semaphore_wait(barrier, ncache - 1)
    q_copies = {s: send(0, s, q_all.at[me], q_all.at[me]) for s in far_first}

    c_k.wait()
    key_new = rotated(row_dot(normed, wk[...])).astype(F32)
    c_v.wait()
    value_new = row_dot(normed, wv[...]).astype(BF16).astype(F32)

    def stacked(block):
        wide_block = block.astype(F32)
        return jnp.concatenate(
            [wide_block[:, g * HEAD_DIM : (g + 1) * HEAD_DIM] for g in range(GROUP)], axis=0
        )

    own_query = stacked(query)
    own_key = jnp.concatenate([key_new] * GROUP, axis=0)
    own_value = jnp.concatenate([value_new] * GROUP, axis=0)
    own_score = jnp.sum(own_query * own_key, axis=-1, keepdims=True) * scale

    c_kc.wait()
    c_vc.wait()
    for s in near_first:
        q_copies[s].wait_recv()

    rows1 = GROUP * seqs
    diag = lax.broadcasted_iota(jnp.int32, (rows1, HEAD_DIM), 0) == lax.broadcasted_iota(
        jnp.int32, (rows1, HEAD_DIM), 1
    )
    blank = jnp.zeros((rows1, HEAD_DIM), F32)
    for pair in range(KV_HEADS // 2):
        lanes = slice(pair * 2 * HEAD_DIM, (pair + 1) * 2 * HEAD_DIM)
        first = stacked(q_all[2 * pair])
        second = stacked(q_all[2 * pair + 1])
        both = jnp.concatenate(
            [
                jnp.concatenate([first, blank], axis=1),
                jnp.concatenate([blank, second], axis=1),
            ],
            axis=0,
        ).astype(BF16)
        scores = jnp.full((rows2, slots), LOW, F32)
        for b in range(0, seqs, 2):
            keys = kc[b : b + 2, :, lanes].reshape(2 * slots, 2 * HEAD_DIM)
            part = lax.dot_general(
                both, keys, (((1,), (1,)), ((), ())), preferred_element_type=F32
            )
            scores = jnp.where(row_seq == b, part[:, :slots], scores)
            scores = jnp.where(row_seq == b + 1, part[:, slots:], scores)
        scores = jnp.where(valid, scores * scale, LOW)
        top = jnp.max(scores, axis=-1, keepdims=True)
        weights = jnp.where(valid, jnp.exp(scores - top), 0.0)
        total = jnp.sum(weights, axis=-1, keepdims=True)
        summed = jnp.zeros((rows2, 2 * HEAD_DIM), F32)
        for b in range(0, seqs, 2):
            picked = jnp.concatenate(
                [
                    jnp.where(row_seq == b, weights, 0.0),
                    jnp.where(row_seq == b + 1, weights, 0.0),
                ],
                axis=1,
            ).astype(BF16)
            values = vc[b : b + 2, :, lanes].reshape(2 * slots, 2 * HEAD_DIM)
            summed += row_dot(picked, values)
        some = total > 0.0
        safe = jnp.where(some, total, 1.0)
        level = jnp.where(some, top + jnp.log(safe), LOW)
        summed = summed / safe
        o_send[2 * pair] = summed[:rows1, :HEAD_DIM].astype(BF16)
        o_send[2 * pair + 1] = summed[rows1:, HEAD_DIM:].astype(BF16)
        l_send[2 * pair] = jnp.sum(jnp.where(diag, level[:rows1], 0.0), axis=0, keepdims=True)
        l_send[2 * pair + 1] = jnp.sum(jnp.where(diag, level[rows1:], 0.0), axis=0, keepdims=True)

    l_copies = {s: send(1, s, l_send.at[peers[s]], l_recv.at[s]) for s in far_first}
    o_copies = {s: send(2, s, o_send.at[peers[s]], o_recv.at[s]) for s in far_first}

    def column(row):
        return jnp.sum(jnp.where(diag, row, 0.0), axis=-1, keepdims=True)

    levels = [column(l_send[me])]
    for s in range(1, ncache):
        l_copies[s].wait_recv()
        levels.append(column(l_recv[s]))
    highest = own_score
    for level in levels:
        highest = jnp.maximum(highest, level)
    share = jnp.exp(own_score - highest)
    denominator = share
    joined = share * own_value
    for s in range(ncache):
        share = jnp.exp(levels[s] - highest)
        denominator += share
        if s == 0:
            block = o_send[me]
        else:
            o_copies[s].wait_recv()
            block = o_recv[s]
        joined += share * block.astype(F32)
    joined = joined / denominator
    attended = jnp.concatenate(
        [joined[g * seqs : (g + 1) * seqs] for g in range(GROUP)], axis=1
    ).astype(BF16)

    def features(index):
        return pl.ds(pl.multiple_of(index * feat, feat), feat)

    c_wo.wait()
    p_copies = {}
    for s in far_first:
        p_send[s] = row_dot(attended, wo[:, features(peers[s])]).astype(BF16)
        p_copies[s] = send(3, s, p_send.at[s], p_recv.at[s])
    mid = hid[:, features(me)].astype(F32) + row_dot(attended, wo[:, features(me)])
    for s in near_first:
        p_copies[s].wait_recv()
        mid += p_recv[s].astype(F32)
    mid_low = mid.astype(BF16)
    m_send[...] = mid_low
    m_copies = {s: send(4, s, m_send, m_recv.at[s]) for s in far_first}

    c_mgain.wait()
    c_wg.wait()
    c_wu.wait()
    squares = jnp.zeros((seqs, 1), F32)
    gate = jnp.zeros((seqs, wg.shape[1]), F32)
    upper = jnp.zeros((seqs, wu.shape[1]), F32)
    for s in [0] + near_first:
        if s == 0:
            block = mid_low.astype(F32)
        else:
            m_copies[s].wait_recv()
            block = m_recv[s].astype(F32)
        where = features(sources[s])
        squares += jnp.sum(block * block, axis=-1, keepdims=True)
        low = (block * mgain[:, where].astype(F32)).astype(BF16)
        gate += row_dot(low, wg[where, :])
        upper += row_dot(low, wu[where, :])
    factor = lax.rsqrt(squares / width + EPS)
    gate = gate * factor
    act = (gate / (1.0 + jnp.exp(-gate)) * (upper * factor)).astype(BF16)

    c_wd.wait()
    d_copies = {}
    for s in far_first:
        d_send[s] = row_dot(act, wd[:, features(peers[s])]).astype(BF16)
        d_copies[s] = send(5, s, d_send.at[s], d_recv.at[s])
    result = mid_low.astype(F32) + row_dot(act, wd[:, features(me)])
    for s in near_first:
        d_copies[s].wait_recv()
        result += d_recv[s].astype(F32)
    out_ref[...] = result.astype(BF16)

    for copies in (q_copies, l_copies, o_copies, p_copies, m_copies, d_copies):
        for s in range(1, ncache):
            copies[s].wait_send()


def fused_device(
    hidden_in,
    attn_gain,
    w_query,
    w_key,
    w_value,
    key_cache,
    value_cache,
    write_pos,
    cache_len,
    w_out,
    mlp_gain,
    w_gate,
    w_up,
    w_down,
):
    ncache = lax.axis_size("cache")
    seqs, width = hidden_in.shape
    feat = width // ncache
    rows = GROUP * seqs
    qchunks = 4
    index = np.arange(HEAD_DIM // 2, dtype=np.float32)
    freq = np.float32(10000.0) ** (-(index * np.float32(2.0) / np.float32(HEAD_DIM)))
    freq = np.concatenate([freq, freq]).astype(np.float32)[None, :]
    big = [
        jnp.asarray(freq),
        hidden_in,
        attn_gain.reshape(1, width),
        w_query,
        w_key,
        w_value,
        key_cache,
        value_cache,
        w_out,
        mlp_gain.reshape(1, width),
        w_gate,
        w_up,
        w_down,
    ]
    vmem = pltpu.VMEM
    scratch = [vmem(x.shape, x.dtype) for x in big] + [
        vmem((ncache, seqs, w_query.shape[1]), BF16),
        vmem((ncache, rows, HEAD_DIM), BF16),
        vmem((ncache, rows, HEAD_DIM), BF16),
        vmem((ncache, 1, HEAD_DIM), F32),
        vmem((ncache, 1, HEAD_DIM), F32),
        vmem((ncache, seqs, feat), BF16),
        vmem((ncache, seqs, feat), BF16),
        vmem((seqs, feat), BF16),
        vmem((ncache, seqs, feat), BF16),
        vmem((ncache, seqs, feat), BF16),
        vmem((ncache, seqs, feat), BF16),
        pltpu.SemaphoreType.DMA((12,)),
        pltpu.SemaphoreType.DMA((qchunks,)),
        pltpu.SemaphoreType.DMA((6, ncache)),
        pltpu.SemaphoreType.DMA((6, ncache)),
    ]
    return pl.pallas_call(
        functools.partial(layer_kernel, ncache, qchunks),
        out_shape=jax.ShapeDtypeStruct((seqs, feat), BF16),
        in_specs=[pl.BlockSpec(memory_space=pltpu.SMEM)] * 2
        + [pl.BlockSpec(memory_space=pl.ANY)] * len(big),
        out_specs=pl.BlockSpec(memory_space=pltpu.VMEM),
        scratch_shapes=scratch,
        compiler_params=pltpu.CompilerParams(
            collective_id=0, has_side_effects=True, vmem_limit_bytes=60 * 1024 * 1024
        ),
    )(write_pos, cache_len, *big)


def fits(ncache, seqs_dev, slots_dev):
    return ncache == KV_HEADS and seqs_dev == 8 and slots_dev == HEAD_DIM


def combined_all(value, axis, join):
    pieces = jax.tree.map(lambda part: lax.all_gather(part, axis), value)
    head = jax.tree.map(lambda part: part[0], pieces)
    tail = jax.tree.map(lambda part: part[1:], pieces)
    running, _ = lax.scan(lambda running, piece: (join(running, piece), None), head, tail)
    return running


def rms_norm(values, gain):
    wide = values.astype(jnp.float32)
    spread = jnp.mean(wide * wide, axis=-1, keepdims=True)
    return (wide * lax.rsqrt(spread + 1e-05) * gain.astype(jnp.float32)).astype(jnp.bfloat16)


def rotate(heads, position):
    half = heads.shape[-1] // 2
    freq = 10000.0 ** (-(jnp.arange(half, dtype=jnp.float32) * 2.0 / heads.shape[-1]))
    angle = position.astype(jnp.float32)[:, None] * freq[None, :]
    cosine = jnp.cos(angle)[:, None, :]
    sine = jnp.sin(angle)[:, None, :]
    first = heads[..., :half]
    second = heads[..., half:]
    return jnp.concatenate(
        [first * cosine - second * sine, second * cosine + first * sine], axis=-1
    )


def per_device(
    hidden_in,
    attn_gain,
    w_query,
    w_key,
    w_value,
    key_cache,
    value_cache,
    write_pos,
    cache_len,
    w_out,
    mlp_gain,
    w_gate,
    w_up,
    w_down,
):
    if fits(lax.axis_size("cache"), hidden_in.shape[0], key_cache.shape[1]):
        return fused_device(
            hidden_in,
            attn_gain,
            w_query,
            w_key,
            w_value,
            key_cache,
            value_cache,
            write_pos,
            cache_len,
            w_out,
            mlp_gain,
            w_gate,
            w_up,
            w_down,
        )
    seqs = hidden_in.shape[0]
    embedding_width = hidden_in.shape[1]
    ncache = lax.axis_size("cache")
    position_index = lax.axis_index("cache")
    slots_dev = key_cache.shape[1]
    window = slots_dev * ncache
    group = HEADS // KV_HEADS
    scale = 1.0 / HEAD_DIM**0.5
    feature_width = embedding_width // ncache
    normed = rms_norm(hidden_in, attn_gain)
    query_slice = jnp.dot(normed, w_query, preferred_element_type=jnp.float32).astype(jnp.bfloat16)
    key_part = jnp.dot(normed, w_key, preferred_element_type=jnp.float32).astype(jnp.bfloat16)
    value_part = jnp.dot(normed, w_value, preferred_element_type=jnp.float32).astype(jnp.bfloat16)
    query_raw, key_raw, value_new = (
        lax.all_gather(query_slice, "cache", axis=1, tiled=True),
        lax.all_gather(key_part, "cache", axis=1, tiled=True),
        lax.all_gather(value_part, "cache", axis=1, tiled=True),
    )
    query = rotate(query_raw.astype(jnp.float32).reshape(seqs, HEADS, HEAD_DIM), write_pos).astype(
        jnp.bfloat16
    )
    fresh_key_row = rotate(
        key_raw.astype(jnp.float32).reshape(seqs, KV_HEADS, HEAD_DIM), write_pos
    ).astype(jnp.bfloat16)
    value_heads = value_new.reshape(seqs, KV_HEADS, HEAD_DIM)
    slots = position_index * slots_dev + jnp.arange(slots_dev, dtype=jnp.int32)
    dist = (write_pos[:, None] - 1 - slots[None, :]) % window + 1
    valid = dist <= cache_len[:, None]
    owner = write_pos % window // slots_dev == position_index
    query_head_group = query.reshape(seqs, KV_HEADS, group, HEAD_DIM)
    keys = key_cache.reshape(seqs, slots_dev, KV_HEADS, HEAD_DIM)
    values = value_cache.reshape(seqs, slots_dev, KV_HEADS, HEAD_DIM)
    scores = (
        jnp.einsum("bkgd,bwkd->bkgw", query_head_group, keys, preferred_element_type=jnp.float32)
        * scale
    )
    own = (
        jnp.einsum(
            "vyjf,vyf->vyj", query_head_group, fresh_key_row, preferred_element_type=jnp.float32
        )
        * scale
    )
    scores = jnp.where(valid[:, None, None, :], scores, -1e30)
    own = jnp.where(owner[:, None, None], own, -1e30)
    top = jnp.maximum(jnp.max(scores, axis=-1), own)
    weights = jnp.where(valid[:, None, None, :], jnp.exp(scores - top[..., None]), 0.0)
    own_weight = jnp.where(owner[:, None, None], jnp.exp(own - top), 0.0)
    total = jnp.sum(weights, axis=-1) + own_weight
    own_low = lax.optimization_barrier(own_weight.astype(jnp.bfloat16)).astype(jnp.float32)
    reduced_total = jnp.einsum(
        "bkgw,bwkd->bkgd", weights.astype(jnp.bfloat16), values, preferred_element_type=jnp.float32
    )
    reduced_total = (
        reduced_total + own_low[..., None] * value_heads.astype(jnp.float32)[:, :, None, :]
    )
    top_flat = top.reshape(seqs, HEADS)
    total_flat = total.reshape(seqs, HEADS)
    summed_flat = reduced_total.reshape(seqs, HEADS, HEAD_DIM)

    def combine(first, second):
        top_a, total_a, sum_a = first
        top_b, total_b, sum_b = second
        larger = jnp.maximum(top_a, top_b)
        factor_a = jnp.exp(top_a - larger)
        factor_b = jnp.exp(top_b - larger)
        merged = sum_a * factor_a[..., None] + sum_b * factor_b[..., None]
        return (larger, total_a * factor_a + total_b * factor_b, merged)

    merged_top, merged_total, merged_sum = combined_all(
        (top_flat, total_flat, summed_flat), "cache", combine
    )
    attended_heads_joined = (
        (merged_sum / merged_total[..., None]).reshape(seqs, HEADS * HEAD_DIM).astype(jnp.bfloat16)
    )
    attended = lax.dynamic_slice_in_dim(
        attended_heads_joined, position_index * feature_width, feature_width, 1
    )
    projected = jnp.dot(attended, w_out, preferred_element_type=jnp.float32)
    projected_sum = lax.psum(projected.astype(jnp.bfloat16), "cache").astype(jnp.float32)
    mid = (hidden_in.astype(jnp.float32) + projected_sum).astype(jnp.bfloat16)
    normed_mid = rms_norm(mid, mlp_gain)
    mid_own = lax.dynamic_slice_in_dim(mid, position_index * feature_width, feature_width, 1)
    gate = jnp.dot(normed_mid, w_gate, preferred_element_type=jnp.float32)
    upper = jnp.dot(normed_mid, w_up, preferred_element_type=jnp.float32)
    act = (jax.nn.silu(gate) * upper).astype(jnp.bfloat16)
    down = jnp.dot(act, w_down, preferred_element_type=jnp.float32)
    down_own = lax.psum_scatter(
        down.astype(jnp.bfloat16), "cache", scatter_dimension=1, tiled=True
    ).astype(jnp.float32)
    return (mid_own.astype(jnp.float32) + down_own).astype(jnp.bfloat16)


def solution(mesh):
    in_specs = (
        P("batch", None),
        P(),
        P(None, "cache"),
        P(None, "cache"),
        P(None, "cache"),
        P("batch", "cache", None),
        P("batch", "cache", None),
        P("batch"),
        P("batch"),
        P("cache", None),
        P(),
        P(None, "cache"),
        P(None, "cache"),
        P("cache", None),
    )
    out_specs = P("batch", "cache")
    return jax.shard_map(
        per_device, mesh=mesh, in_specs=in_specs, out_specs=out_specs, check_vma=False
    )
```

```python
import functools

import jax
import jax.numpy as jnp
import numpy as np
from jax import lax
from jax.experimental import pallas as pl
from jax.experimental.pallas import tpu as pltpu
from jax.sharding import PartitionSpec as P

HEADS = 32
KV_HEADS = 8
HEAD_DIM = 128
GROUP = HEADS // KV_HEADS
EPS = 1e-05
LOW = -1e30
MESH = pl.DeviceIdType.MESH
F32 = jnp.float32
BF16 = jnp.bfloat16


def row_dot(left, right):
    return jnp.dot(left, right, preferred_element_type=F32)


def layer_kernel(
    ncache,
    qchunks,
    pos_s,
    len_s,
    freq_h,
    hid_h,
    again_h,
    wq_h,
    wk_h,
    wv_h,
    kc_h,
    vc_h,
    wo_h,
    mgain_h,
    wg_h,
    wu_h,
    wd_h,
    out_ref,
    freq,
    hid,
    again,
    wq,
    wkv,
    kc,
    vc,
    wo,
    mgain,
    wgu,
    wd,
    q_all,
    o_send,
    o_recv,
    l_send,
    l_recv,
    p_send,
    p_recv,
    m_send,
    m_recv,
    d_send,
    d_recv,
    mgain2,
    local_sem,
    q_sem,
    send_sem,
    recv_sem,
):
    me = lax.axis_index("cache")
    line = lax.axis_index("batch")
    seqs, width = hid.shape
    feat = width // ncache
    slots = kc.shape[1]
    window = slots * ncache
    depth = width // qchunks
    scale = 1.0 / HEAD_DIM**0.5
    peers = [lax.rem(me + s, ncache) for s in range(ncache)]
    sources = [lax.rem(me - s + ncache, ncache) for s in range(ncache)]
    half = ncache // 2
    far_first = sorted(range(1, ncache), key=lambda s: (-min(s, ncache - s), s))
    near_first = far_first[::-1]

    def load(i, src, dst):
        copy = pltpu.make_async_copy(src, dst, local_sem.at[i])
        copy.start()
        return copy

    c_hid = load(0, hid_h, hid)
    c_again = load(1, again_h, again)
    c_freq = load(2, freq_h, freq)
    c_mgain = load(3, mgain_h, mgain)
    c_q = []
    for i in range(qchunks):
        rows = pl.ds(i * depth, depth)
        copy = pltpu.make_async_copy(wq_h.at[rows, :], wq.at[rows, :], q_sem.at[i])
        copy.start()
        c_q.append(copy)

    barrier = pltpu.get_barrier_semaphore()
    for s in range(1, ncache):
        pl.semaphore_signal(barrier, inc=1, device_id=(line, peers[s]), device_id_type=MESH)

    def send(phase, s, src, dst):
        copy = pltpu.make_async_remote_copy(
            src_ref=src,
            dst_ref=dst,
            send_sem=send_sem.at[phase, s],
            recv_sem=recv_sem.at[phase, s],
            device_id=(line, peers[s]),
            device_id_type=MESH,
        )
        copy.start()
        return copy

    c_hid.wait()
    c_again.wait()
    c_freq.wait()
    wide = hid[...].astype(F32)
    spread = jnp.mean(wide * wide, axis=-1, keepdims=True)
    normed = (wide * lax.rsqrt(spread + EPS) * again[...].astype(F32).reshape(1, width)).astype(BF16)

    row8 = lax.broadcasted_iota(jnp.int32, (seqs, HEAD_DIM), 0)
    lane8 = lax.broadcasted_iota(jnp.int32, (seqs, HEAD_DIM), 1)
    position = jnp.zeros((seqs, HEAD_DIM), jnp.int32)
    for b in range(seqs):
        position = jnp.where(row8 == b, pos_s[b], position)
    angle = position.astype(F32) * freq[...]
    cosine = jnp.cos(angle)
    sine = jnp.sin(angle)
    sine = jnp.where(lane8 < HEAD_DIM // 2, -sine, sine)

    def rotated(x):
        x = x.astype(BF16).astype(F32)
        return (x * cosine + pltpu.roll(x, HEAD_DIM // 2, 1) * sine).astype(BF16)

    rows2 = 2 * GROUP * seqs
    row_seq = lax.broadcasted_iota(jnp.int32, (rows2, slots), 0) % seqs
    slot = lax.broadcasted_iota(jnp.int32, (rows2, slots), 1) + me * slots
    newest = jnp.zeros((rows2, slots), jnp.int32)
    length = jnp.zeros((rows2, slots), jnp.int32)
    for b in range(seqs):
        newest = jnp.where(row_seq == b, lax.rem(pos_s[b] - 1 + window, window), newest)
        length = jnp.where(row_seq == b, len_s[b], length)
    dist = newest - slot
    dist = jnp.where(dist < 0, dist + window, dist) + 1
    valid = dist <= length

    q_raw = jnp.zeros((seqs, wq.shape[1]), F32)
    for i in range(qchunks):
        c_q[i].wait()
        q_raw += row_dot(normed[:, i * depth : (i + 1) * depth], wq[i * depth : (i + 1) * depth, :])
    head = wk_h.shape[1]
    c_k = load(4, wk_h, wkv.at[:, pl.ds(0, head)])
    c_v = load(5, wv_h, wkv.at[:, pl.ds(head, head)])
    c_kc = load(6, kc_h, kc)
    c_vc = load(7, vc_h, vc)
    query = jnp.concatenate(
        [rotated(q_raw[:, g * HEAD_DIM : (g + 1) * HEAD_DIM]) for g in range(GROUP)], axis=1
    )
    q_all[me] = query
    pl.semaphore_wait(barrier, ncache - 1)
    q_copies = {s: send(0, s, q_all.at[me], q_all.at[me]) for s in near_first}

    c_wo = load(8, wo_h, wo)
    c_k.wait()
    c_v.wait()
    fresh = row_dot(normed, wkv[...])
    key_new = rotated(fresh[:, :head]).astype(F32)
    value_new = fresh[:, head:].astype(BF16).astype(F32)

    def stacked(block):
        wide_block = block.astype(F32)
        return jnp.concatenate(
            [wide_block[:, g * HEAD_DIM : (g + 1) * HEAD_DIM] for g in range(GROUP)], axis=0
        )

    own_query = stacked(query)
    own_key = jnp.concatenate([key_new] * GROUP, axis=0)
    own_value = jnp.concatenate([value_new] * GROUP, axis=0)
    own_score = jnp.sum(own_query * own_key, axis=-1, keepdims=True) * scale

    c_mgain.wait()
    gains = mgain[...].astype(F32).reshape(1, width)
    mgain2[...] = jnp.broadcast_to(gains, mgain2.shape)
    c_kc.wait()
    c_vc.wait()
    for s in near_first:
        q_copies[s].wait_recv()

    ffw = wg_h.shape[1]
    c_wg = load(9, wg_h, wgu.at[:, pl.ds(0, ffw)])
    c_wu = load(10, wu_h, wgu.at[:, pl.ds(ffw, ffw)])
    rows1 = GROUP * seqs
    diag = lax.broadcasted_iota(jnp.int32, (rows1, HEAD_DIM), 0) == lax.broadcasted_iota(
        jnp.int32, (rows1, HEAD_DIM), 1
    )
    blank = jnp.zeros((rows1, HEAD_DIM), F32)
    for pair in range(KV_HEADS // 2):
        lanes = slice(pair * 2 * HEAD_DIM, (pair + 1) * 2 * HEAD_DIM)
        first = stacked(q_all[2 * pair])
        second = stacked(q_all[2 * pair + 1])
        both = jnp.concatenate(
            [
                jnp.concatenate([first, blank], axis=1),
                jnp.concatenate([blank, second], axis=1),
            ],
            axis=0,
        ).astype(BF16)
        scores = jnp.full((rows2, slots), LOW, F32)
        for b in range(0, seqs, 2):
            keys = kc[b : b + 2, :, lanes].reshape(2 * slots, 2 * HEAD_DIM)
            part = lax.dot_general(
                both, keys, (((1,), (1,)), ((), ())), preferred_element_type=F32
            )
            scores = jnp.where(row_seq == b, part[:, :slots], scores)
            scores = jnp.where(row_seq == b + 1, part[:, slots:], scores)
        scores = jnp.where(valid, scores * scale, LOW)
        top = jnp.max(scores, axis=-1, keepdims=True)
        weights = jnp.where(valid, jnp.exp(scores - top), 0.0)
        total = jnp.sum(weights, axis=-1, keepdims=True)
        summed = jnp.zeros((rows2, 2 * HEAD_DIM), F32)
        for b in range(0, seqs, 2):
            picked = jnp.concatenate(
                [
                    jnp.where(row_seq == b, weights, 0.0),
                    jnp.where(row_seq == b + 1, weights, 0.0),
                ],
                axis=1,
            ).astype(BF16)
            values = vc[b : b + 2, :, lanes].reshape(2 * slots, 2 * HEAD_DIM)
            summed += row_dot(picked, values)
        some = total > 0.0
        safe = jnp.where(some, total, 1.0)
        level = jnp.where(some, top + jnp.log(safe), LOW)
        summed = summed / safe
        o_send[2 * pair] = summed[:rows1, :HEAD_DIM].astype(BF16)
        o_send[2 * pair + 1] = summed[rows1:, HEAD_DIM:].astype(BF16)
        l_send[2 * pair] = jnp.sum(jnp.where(diag, level[:rows1], 0.0), axis=0, keepdims=True)
        l_send[2 * pair + 1] = jnp.sum(jnp.where(diag, level[rows1:], 0.0), axis=0, keepdims=True)

    l_copies = {s: send(1, s, l_send.at[peers[s]], l_recv.at[s]) for s in near_first}
    o_copies = {s: send(2, s, o_send.at[peers[s]], o_recv.at[s]) for s in near_first}

    def column(row):
        return jnp.sum(jnp.where(diag, row, 0.0), axis=-1, keepdims=True)

    levels = [column(l_send[me])]
    for s in range(1, ncache):
        l_copies[s].wait_recv()
        levels.append(column(l_recv[s]))
    highest = own_score
    for level in levels:
        highest = jnp.maximum(highest, level)
    share = jnp.exp(own_score - highest)
    denominator = share
    joined = share * own_value
    for s in range(ncache):
        share = jnp.exp(levels[s] - highest)
        denominator += share
        if s == 0:
            block = o_send[me]
        else:
            o_copies[s].wait_recv()
            block = o_recv[s]
        joined += share * block.astype(F32)
    joined = joined / denominator
    attended = jnp.concatenate(
        [joined[g * seqs : (g + 1) * seqs] for g in range(GROUP)], axis=1
    ).astype(BF16)

    def features(index):
        return pl.ds(pl.multiple_of(index * feat, feat), feat)

    c_wd = load(11, wd_h, wd)
    c_wo.wait()
    p_copies = {}
    for s in near_first:
        p_send[s] = row_dot(attended, wo[:, features(peers[s])]).astype(BF16)
        p_copies[s] = send(3, s, p_send.at[s], p_recv.at[s])
    mid = hid[:, features(me)].astype(F32) + row_dot(attended, wo[:, features(me)])
    for s in near_first:
        p_copies[s].wait_recv()
        mid += p_recv[s].astype(F32)
    mid_low = mid.astype(BF16)
    m_send[...] = mid_low
    m_copies = {s: send(4, s, m_send, m_recv.at[s]) for s in near_first}

    c_wg.wait()
    c_wu.wait()
    squares = jnp.zeros((seqs, 1), F32)
    both = jnp.zeros((seqs, 2 * ffw), F32)
    for s in [0] + near_first:
        if s == 0:
            block = mid_low.astype(F32)
        else:
            m_copies[s].wait_recv()
            block = m_recv[s].astype(F32)
        where = features(sources[s])
        squares += jnp.sum(block * block, axis=-1, keepdims=True)
        low = (block * mgain2[:, where]).astype(BF16)
        both += row_dot(low, wgu[where, :])
    factor = lax.rsqrt(squares / width + EPS)
    both = both * factor
    gate = both[:, :ffw]
    act = (gate / (1.0 + jnp.exp(-gate)) * both[:, ffw:]).astype(BF16)

    c_wd.wait()
    d_copies = {}
    for s in near_first:
        d_send[s] = row_dot(act, wd[:, features(peers[s])]).astype(BF16)
        d_copies[s] = send(5, s, d_send.at[s], d_recv.at[s])
    result = mid_low.astype(F32) + row_dot(act, wd[:, features(me)])
    for s in near_first:
        d_copies[s].wait_recv()
        result += d_recv[s].astype(F32)
    out_ref[...] = result.astype(BF16)

    for copies in (q_copies, l_copies, o_copies, p_copies, m_copies, d_copies):
        for s in range(1, ncache):
            copies[s].wait_send()


def fused_device(
    hidden_in,
    attn_gain,
    w_query,
    w_key,
    w_value,
    key_cache,
    value_cache,
    write_pos,
    cache_len,
    w_out,
    mlp_gain,
    w_gate,
    w_up,
    w_down,
):
    ncache = lax.axis_size("cache")
    seqs, width = hidden_in.shape
    feat = width // ncache
    rows = GROUP * seqs
    qchunks = 4
    index = np.arange(HEAD_DIM // 2, dtype=np.float32)
    freq = np.float32(10000.0) ** (-(index * np.float32(2.0) / np.float32(HEAD_DIM)))
    freq = np.concatenate([freq, freq]).astype(np.float32)[None, :]
    big = [
        jnp.asarray(freq),
        hidden_in,
        attn_gain,
        w_query,
        w_key,
        w_value,
        key_cache,
        value_cache,
        w_out,
        mlp_gain,
        w_gate,
        w_up,
        w_down,
    ]
    vmem = pltpu.VMEM
    shapes = [x.shape for x in big]
    joint = lambda shape: (shape[0], 2 * shape[1])
    shapes[4:6] = [joint(w_key.shape)]
    shapes[9:11] = [joint(w_gate.shape)]
    kinds = [F32] + [BF16] * (len(shapes) - 1)
    scratch = [vmem(shape, kind) for shape, kind in zip(shapes, kinds)] + [
        vmem((ncache, seqs, w_query.shape[1]), BF16),
        vmem((ncache, rows, HEAD_DIM), BF16),
        vmem((ncache, rows, HEAD_DIM), BF16),
        vmem((ncache, 1, HEAD_DIM), F32),
        vmem((ncache, 1, HEAD_DIM), F32),
        vmem((ncache, seqs, feat), BF16),
        vmem((ncache, seqs, feat), BF16),
        vmem((seqs, feat), BF16),
        vmem((ncache, seqs, feat), BF16),
        vmem((ncache, seqs, feat), BF16),
        vmem((ncache, seqs, feat), BF16),
        vmem((seqs, width), F32),
        pltpu.SemaphoreType.DMA((12,)),
        pltpu.SemaphoreType.DMA((qchunks,)),
        pltpu.SemaphoreType.DMA((6, ncache)),
        pltpu.SemaphoreType.DMA((6, ncache)),
    ]
    return pl.pallas_call(
        functools.partial(layer_kernel, ncache, qchunks),
        out_shape=jax.ShapeDtypeStruct((seqs, feat), BF16),
        in_specs=[pl.BlockSpec(memory_space=pltpu.SMEM)] * 2
        + [pl.BlockSpec(memory_space=pl.ANY)] * len(big),
        out_specs=pl.BlockSpec(memory_space=pltpu.VMEM),
        scratch_shapes=scratch,
        compiler_params=pltpu.CompilerParams(
            collective_id=0, has_side_effects=True, vmem_limit_bytes=60 * 1024 * 1024
        ),
    )(write_pos, cache_len, *big)


def fits(ncache, seqs_dev, slots_dev):
    return ncache == KV_HEADS and seqs_dev == 8 and slots_dev == HEAD_DIM


def combined_all(value, axis, join):
    pieces = jax.tree.map(lambda part: lax.all_gather(part, axis), value)
    head = jax.tree.map(lambda part: part[0], pieces)
    tail = jax.tree.map(lambda part: part[1:], pieces)
    running, _ = lax.scan(lambda running, piece: (join(running, piece), None), head, tail)
    return running


def rms_norm(values, gain):
    wide = values.astype(jnp.float32)
    spread = jnp.mean(wide * wide, axis=-1, keepdims=True)
    return (wide * lax.rsqrt(spread + 1e-05) * gain.astype(jnp.float32)).astype(jnp.bfloat16)


def rotate(heads, position):
    half = heads.shape[-1] // 2
    freq = 10000.0 ** (-(jnp.arange(half, dtype=jnp.float32) * 2.0 / heads.shape[-1]))
    angle = position.astype(jnp.float32)[:, None] * freq[None, :]
    cosine = jnp.cos(angle)[:, None, :]
    sine = jnp.sin(angle)[:, None, :]
    first = heads[..., :half]
    second = heads[..., half:]
    return jnp.concatenate(
        [first * cosine - second * sine, second * cosine + first * sine], axis=-1
    )


def per_device(
    hidden_in,
    attn_gain,
    w_query,
    w_key,
    w_value,
    key_cache,
    value_cache,
    write_pos,
    cache_len,
    w_out,
    mlp_gain,
    w_gate,
    w_up,
    w_down,
):
    if fits(lax.axis_size("cache"), hidden_in.shape[0], key_cache.shape[1]):
        return fused_device(
            hidden_in,
            attn_gain,
            w_query,
            w_key,
            w_value,
            key_cache,
            value_cache,
            write_pos,
            cache_len,
            w_out,
            mlp_gain,
            w_gate,
            w_up,
            w_down,
        )
    seqs = hidden_in.shape[0]
    embedding_width = hidden_in.shape[1]
    ncache = lax.axis_size("cache")
    position_index = lax.axis_index("cache")
    slots_dev = key_cache.shape[1]
    window = slots_dev * ncache
    group = HEADS // KV_HEADS
    scale = 1.0 / HEAD_DIM**0.5
    feature_width = embedding_width // ncache
    normed = rms_norm(hidden_in, attn_gain)
    query_slice = jnp.dot(normed, w_query, preferred_element_type=jnp.float32).astype(jnp.bfloat16)
    key_part = jnp.dot(normed, w_key, preferred_element_type=jnp.float32).astype(jnp.bfloat16)
    value_part = jnp.dot(normed, w_value, preferred_element_type=jnp.float32).astype(jnp.bfloat16)
    query_raw, key_raw, value_new = (
        lax.all_gather(query_slice, "cache", axis=1, tiled=True),
        lax.all_gather(key_part, "cache", axis=1, tiled=True),
        lax.all_gather(value_part, "cache", axis=1, tiled=True),
    )
    query = rotate(query_raw.astype(jnp.float32).reshape(seqs, HEADS, HEAD_DIM), write_pos).astype(
        jnp.bfloat16
    )
    fresh_key_row = rotate(
        key_raw.astype(jnp.float32).reshape(seqs, KV_HEADS, HEAD_DIM), write_pos
    ).astype(jnp.bfloat16)
    value_heads = value_new.reshape(seqs, KV_HEADS, HEAD_DIM)
    slots = position_index * slots_dev + jnp.arange(slots_dev, dtype=jnp.int32)
    dist = (write_pos[:, None] - 1 - slots[None, :]) % window + 1
    valid = dist <= cache_len[:, None]
    owner = write_pos % window // slots_dev == position_index
    query_head_group = query.reshape(seqs, KV_HEADS, group, HEAD_DIM)
    keys = key_cache.reshape(seqs, slots_dev, KV_HEADS, HEAD_DIM)
    values = value_cache.reshape(seqs, slots_dev, KV_HEADS, HEAD_DIM)
    scores = (
        jnp.einsum("bkgd,bwkd->bkgw", query_head_group, keys, preferred_element_type=jnp.float32)
        * scale
    )
    own = (
        jnp.einsum(
            "vyjf,vyf->vyj", query_head_group, fresh_key_row, preferred_element_type=jnp.float32
        )
        * scale
    )
    scores = jnp.where(valid[:, None, None, :], scores, -1e30)
    own = jnp.where(owner[:, None, None], own, -1e30)
    top = jnp.maximum(jnp.max(scores, axis=-1), own)
    weights = jnp.where(valid[:, None, None, :], jnp.exp(scores - top[..., None]), 0.0)
    own_weight = jnp.where(owner[:, None, None], jnp.exp(own - top), 0.0)
    total = jnp.sum(weights, axis=-1) + own_weight
    own_low = lax.optimization_barrier(own_weight.astype(jnp.bfloat16)).astype(jnp.float32)
    reduced_total = jnp.einsum(
        "bkgw,bwkd->bkgd", weights.astype(jnp.bfloat16), values, preferred_element_type=jnp.float32
    )
    reduced_total = (
        reduced_total + own_low[..., None] * value_heads.astype(jnp.float32)[:, :, None, :]
    )
    top_flat = top.reshape(seqs, HEADS)
    total_flat = total.reshape(seqs, HEADS)
    summed_flat = reduced_total.reshape(seqs, HEADS, HEAD_DIM)

    def combine(first, second):
        top_a, total_a, sum_a = first
        top_b, total_b, sum_b = second
        larger = jnp.maximum(top_a, top_b)
        factor_a = jnp.exp(top_a - larger)
        factor_b = jnp.exp(top_b - larger)
        merged = sum_a * factor_a[..., None] + sum_b * factor_b[..., None]
        return (larger, total_a * factor_a + total_b * factor_b, merged)

    merged_top, merged_total, merged_sum = combined_all(
        (top_flat, total_flat, summed_flat), "cache", combine
    )
    attended_heads_joined = (
        (merged_sum / merged_total[..., None]).reshape(seqs, HEADS * HEAD_DIM).astype(jnp.bfloat16)
    )
    attended = lax.dynamic_slice_in_dim(
        attended_heads_joined, position_index * feature_width, feature_width, 1
    )
    projected = jnp.dot(attended, w_out, preferred_element_type=jnp.float32)
    projected_sum = lax.psum(projected.astype(jnp.bfloat16), "cache").astype(jnp.float32)
    mid = (hidden_in.astype(jnp.float32) + projected_sum).astype(jnp.bfloat16)
    normed_mid = rms_norm(mid, mlp_gain)
    mid_own = lax.dynamic_slice_in_dim(mid, position_index * feature_width, feature_width, 1)
    gate = jnp.dot(normed_mid, w_gate, preferred_element_type=jnp.float32)
    upper = jnp.dot(normed_mid, w_up, preferred_element_type=jnp.float32)
    act = (jax.nn.silu(gate) * upper).astype(jnp.bfloat16)
    down = jnp.dot(act, w_down, preferred_element_type=jnp.float32)
    down_own = lax.psum_scatter(
        down.astype(jnp.bfloat16), "cache", scatter_dimension=1, tiled=True
    ).astype(jnp.float32)
    return (mid_own.astype(jnp.float32) + down_own).astype(jnp.bfloat16)


def solution(mesh):
    in_specs = (
        P("batch", None),
        P(),
        P(None, "cache"),
        P(None, "cache"),
        P(None, "cache"),
        P("batch", "cache", None),
        P("batch", "cache", None),
        P("batch"),
        P("batch"),
        P("cache", None),
        P(),
        P(None, "cache"),
        P(None, "cache"),
        P("cache", None),
    )
    out_specs = P("batch", "cache")
    return jax.shard_map(
        per_device, mesh=mesh, in_specs=in_specs, out_specs=out_specs, check_vma=False
    )
```
